32 devices in a mesh: tm: 4 (over y, x), row: 8 (over z, core).
Axes of the slice: x: 2, y: 2, z: 4, core: 2. Of those that a mesh axis runs over, the one named last changes fastest.
Arguments:
- coupling: float32 [4, 8192, 8192], P('tm', 'row'), may hold values from -0.0625 to 0.0625
- damping: float32 [4, 8192], P('tm', 'row'), may hold values from 0.5 to 3
- forcing: float32 [4, 8, 8192], P('tm', None, 'row'), may hold values from -6 to 6
- initial: float32 [8, 8192], P(None, 'row'), may hold values from -6 to 6
- counts: int32 [4], P('tm'), may hold values from 1 to 8
Outputs:
- states: float32 [4, 8, 8192], P('tm', None, 'row')
The draws below stay inside these ranges and needn't reach their ends.
All inputs are finite; a program needn't handle non-finite values.
Results may differ from the reference program's by a relative error of at most 0.00013.
Values sent between devices are 32-bit elements; how exact they have to be, the bound alone decides.
No kernel may reach another device: no remote copies, remote signals or barrier semaphores. Data moves between devices by JAX's collectives and lax.ppermute only.
A program may use at most 128 MiB of HBM per device.

```python
import math
import jax
import jax.numpy as jnp
from jax import lax

N = 8192
KRYLOV = 2
MEMBERS = 8
SLABS = 4


def plant(values, key, smallest, high):
    spot = [jax.random.randint(jax.random.fold_in(key, axis), (), 0, length) for axis, length in enumerate(values.shape)]
    main_axis = values.shape.index(max(values.shape))
    beside = spot[:main_axis] + [(spot[main_axis] + 1) % values.shape[main_axis]] + spot[main_axis + 1:]
    return values.at[tuple(spot)].set(smallest).at[tuple(beside)].set(high)


def levels(rng, shape, cuts, least, top_value):
    loudness, own = 1.0, jax.random.fold_in(rng, 6)
    for axis_at, blocks in cuts:
        steps = jnp.exp(jax.random.uniform(jax.random.fold_in(own, axis_at), (blocks,), jnp.float32, least / len(cuts), top_value / len(cuts)))
        loudness = loudness * jnp.repeat(steps, shape[axis_at] // blocks).reshape([-1 if axis == axis_at else 1 for axis in range(len(shape))])
    return loudness


def scatter_about(own_key, shape, scale, reach, cuts=(), kind=jnp.bfloat16):
    values = scale * jax.random.normal(own_key, shape, jnp.float32)
    if cuts:
        values = values * levels(own_key, shape, cuts, -0.22, 0.18)
    return jnp.clip(values, -reach, reach).astype(kind)


def setup_inputs(seed: int = 0) -> dict:
    splits = jax.random.split(jax.random.key(seed), 6)
    return {
        "coupling": scatter_about(splits[0], (SLABS, N, N), N ** -0.5, 0.0625, ((0, 4), (1, 8)), jnp.float32),
        "damping": jnp.clip(jnp.exp(math.log(3.0) - 1.7917595 * jax.random.uniform(splits[1], (SLABS, N), jnp.float32) ** levels(splits[1], (SLABS, N), ((0, 4), (1, 8)), -0.2, 0.2)), 0.5, 3.0),
        "forcing": scatter_about(splits[2], (SLABS, MEMBERS, N), 1.0, 6.0, ((0, 4), (2, 8)), jnp.float32),
        "initial": scatter_about(splits[3], (MEMBERS, N), 1.0, 6.0, ((1, 8),), jnp.float32),
        "counts": plant(jax.random.randint(splits[4], (SLABS,), 1, 9), jax.random.fold_in(splits[4], 1), 1, 8).astype(jnp.int32),
    }


time_step = 0.125
epsilon = 1e-06
squarings = 5
taylor_terms = 12
highest = lax.Precision.HIGHEST

def matrix_exponential(matrix):
    scaled = matrix / 2.0 ** squarings
    dimension = matrix.shape[-1]
    identity = jnp.broadcast_to(jnp.eye(dimension, dtype=jnp.float32), matrix.shape)
    result = identity
    for degree in range(taylor_terms, 0, -1):
        result = identity + jnp.einsum('bij,bjk->bik', scaled, result, precision=highest) / degree
    for repeat in range(squarings):
        result = jnp.einsum('bij,bjk->bik', result, result, precision=highest)
    return result

def exponent_block(hessenberg, step_size):
    members = hessenberg.shape[0]
    augmented = jnp.zeros((members, KRYLOV + 1, KRYLOV + 1), jnp.float32)
    augmented = augmented.at[:, :KRYLOV, :KRYLOV].set(step_size * hessenberg)
    augmented = augmented.at[:, 0, KRYLOV].set(1.0)
    return matrix_exponential(augmented)

def apply_operator(vectors, coupling, damping):
    product = lax.dot_general(vectors, coupling, (((1,), (1,)), ((), ())), precision=highest, preferred_element_type=jnp.float32)
    return product - damping * vectors

def arnoldi(vectors, coupling, damping):
    members = vectors.shape[0]
    extent = vectors.shape[1]
    start_norm = jnp.sqrt(lax.optimization_barrier(jnp.sum(vectors * vectors, axis=1)) + epsilon)
    krylov_basis = jnp.zeros((KRYLOV, members, extent), jnp.float32).at[0].set(vectors / start_norm[:, None])
    hessenberg = jnp.zeros((members, KRYLOV, KRYLOV), jnp.float32)
    for column in range(KRYLOV):
        applied = apply_operator(krylov_basis[column], coupling, damping)
        weights = jnp.einsum('kbn,bn->kb', krylov_basis, applied, precision=highest)
        applied = applied - jnp.einsum('kb,kbn->bn', weights, krylov_basis, precision=highest)
        hessenberg = hessenberg.at[:, :, column].set(weights.T)
        if column + 1 < KRYLOV:
            length = jnp.sqrt(lax.optimization_barrier(jnp.sum(applied * applied, axis=1)) + epsilon)
            krylov_basis = krylov_basis.at[column + 1].set(applied / length[:, None])
            hessenberg = hessenberg.at[:, column + 1, column].set(length)
    return (start_norm, krylov_basis, hessenberg)

def combine_basis(krylov_basis, coefficients):
    return jnp.einsum('kbn,bk->bn', krylov_basis, coefficients, precision=highest)

def reference(coupling, damping, forcing, initial, counts):
    states = []
    carried = initial
    for slab_index in range(SLABS):
        step_size = counts[slab_index].astype(jnp.float32) * time_step
        forcing_norm, forcing_basis, forcing_hessenberg = arnoldi(forcing[slab_index], coupling[slab_index], damping[slab_index])
        forcing_block = exponent_block(forcing_hessenberg, step_size)
        local_part = combine_basis(forcing_basis, (step_size * forcing_norm)[:, None] * forcing_block[:, :KRYLOV, KRYLOV])
        carried_norm, carried_basis, carried_hessenberg = arnoldi(carried, coupling[slab_index], damping[slab_index])
        carried_block = exponent_block(carried_hessenberg, step_size)
        carried = combine_basis(carried_basis, carried_norm[:, None] * carried_block[:, :KRYLOV, 0]) + local_part
        states.append(carried)
    return jnp.stack(states)
```

```python
import functools

import jax
import jax.numpy as jnp
from jax import lax
from jax.experimental import pallas as pl
from jax.experimental.pallas import tpu as pltpu
from jax.sharding import PartitionSpec as P

time_step = 0.125
epsilon = 1e-06
squarings = 5
taylor_terms = 12
MIB = 1 << 20
VMEM = pl.BlockSpec(memory_space=pltpu.VMEM)
SMEM = pl.BlockSpec(memory_space=pltpu.SMEM)
ANY = pl.BlockSpec(memory_space=pl.ANY)
LOAD_WIDTH = 256
LOAD_SLOTS = 6
PIECES = 4


def relative_order(devices):
    return list(range(0, devices, 2)) + list(range(1, devices, 2))


def load_kernel(devices, me_ref, a_ref, *refs):
    piece_refs, (slots, sems) = refs[:PIECES], refs[PIECES:]
    rows, extent = a_ref.shape
    width = slots.shape[2]
    block = extent // devices
    per_block = block // width
    steps = extent // width
    half = devices // 2
    me = me_ref[0]

    def source(step):
        place = step // per_block
        offset = jnp.where(place < half, 2 * place, 2 * (place - half) + 1)
        owner = jnp.bitwise_xor(me, offset)
        start = owner * block + (step % per_block) * width
        return a_ref.at[:, pl.ds(pl.multiple_of(start, width), width)]

    def copy(step):
        slot = step % LOAD_SLOTS
        return pltpu.make_async_copy(source(step), slots.at[slot], sems.at[slot])

    for step in range(min(LOAD_SLOTS, steps)):
        copy(step).start()

    per_piece = steps // PIECES
    for piece, piece_ref in enumerate(piece_refs):

        @pl.loop(0, per_piece)
        def _(inner):
            step = inner + piece * per_piece
            copy(step).wait()
            turned = slots[step % LOAD_SLOTS].T
            high = turned.astype(jnp.bfloat16)
            place = pl.ds(pl.multiple_of(inner * width, width), width)
            piece_ref[0, place, :] = high
            piece_ref[1, place, :] = (turned - high.astype(jnp.float32)).astype(jnp.bfloat16)

            @pl.when(step + LOAD_SLOTS < steps)
            def _():
                copy(step + LOAD_SLOTS).start()


def load_operator(local_coupling, me, devices):
    rows, extent = local_coupling.shape
    width = min(LOAD_WIDTH, extent // devices)

    return pl.pallas_call(
        functools.partial(load_kernel, devices),
        out_shape=(pltpu.VMEM((2, extent // PIECES, rows), jnp.bfloat16),) * PIECES,
        in_specs=[SMEM, ANY],
        out_specs=(VMEM,) * PIECES,
        scratch_shapes=[
            pltpu.VMEM((LOAD_SLOTS, rows, width), jnp.float32),
            pltpu.SemaphoreType.DMA((LOAD_SLOTS,)),
        ],
        compiler_params=pltpu.CompilerParams(vmem_limit_bytes=12 * MIB),
        cost_estimate=pl.CostEstimate(
            flops=1600 * rows * extent, bytes_accessed=4 * rows * extent, transcendentals=0
        ),
        name="load_operator",
    )(me, local_coupling)


def total(first, second):
    def each(block):
        return jnp.sum(jnp.sum(block, axis=0), axis=-1, keepdims=True)

    return each(first) + each(second)


def apply_rows(parts, piece_refs, split_ref, total_ref):
    count = 0
    for part in parts:
        for index in range(part.shape[0]):
            members = part.shape[1]
            block = part[index]
            high = block.astype(jnp.bfloat16)
            split_ref[count, :members] = high.astype(jnp.float32)
            split_ref[count, members:] = block - high.astype(jnp.float32)
            count += 1
    width = split_ref.shape[2]
    total_ref[...] = jnp.zeros_like(total_ref)

    per_piece = count // len(piece_refs)
    for piece, piece_ref in enumerate(piece_refs):

        @pl.loop(0, per_piece)
        def _(inner):
            lhs = split_ref[inner + piece * per_piece].astype(jnp.bfloat16)
            place = pl.ds(pl.multiple_of(inner * width, width), width)
            total_ref[...] += jnp.dot(
                lhs, piece_ref[0, place, :], preferred_element_type=jnp.float32
            ) + jnp.dot(lhs, piece_ref[1, place, :], preferred_element_type=jnp.float32)

    members = total_ref.shape[0] // 2
    return total_ref[:members] + total_ref[members:]


def first_kernel(xa_ref, xb_ref, damping_ref, *refs):
    piece_refs, (out_ref, split_ref, total_ref) = refs[:PIECES], refs[PIECES:]
    xa, xb = xa_ref[...], xb_ref[...]
    norm = jnp.sqrt(total(xa * xa, xb * xb) + epsilon)
    qa, qb = xa / norm[None], xb / norm[None]
    image = apply_rows([qa, qb], piece_refs, split_ref, total_ref)
    out_ref[...] = image - damping_ref[...] * qa[0]


def krylov(xa, xb, wa, wb):
    norm = jnp.sqrt(total(xa * xa, xb * xb) + epsilon)
    qa, qb = xa / norm[None], xb / norm[None]
    first = total(qa * wa, qb * wb)
    ra, rb = wa - first[None] * qa, wb - first[None] * qb
    length = jnp.sqrt(total(ra * ra, rb * rb) + epsilon)
    return norm, first, length, qa, ra / length[None], rb / length[None]


def second_kernel(
    xa_ref, xb_ref, wa_ref, wb_ref, damping_ref, *refs
):
    piece_refs, refs = refs[:PIECES], refs[PIECES:]
    partial_ref, scalars_ref, basis_ref, split_ref, total_ref = refs
    norm, first, length, qa, sa, sb = krylov(xa_ref[...], xb_ref[...], wa_ref[...], wb_ref[...])
    image = apply_rows([sa, sb], piece_refs, split_ref, total_ref)
    image = image - damping_ref[...] * sa[0]
    members = image.shape[0]
    for row, own in ((0, qa[0]), (1, sa[0])):
        inner = jnp.sum(own * image, axis=-1, keepdims=True)
        partial_ref[row] = jnp.broadcast_to(inner, (members, 128))
        basis_ref[row] = own
    for row, value in enumerate((norm, first, length)):
        scalars_ref[row] = jnp.broadcast_to(value, (members, 128))


def exponential(step_size, h00, h01, h10, h11):
    scale = 1.0 / 2.0**squarings
    s00, s01 = step_size * h00 * scale, step_size * h01 * scale
    s10, s11 = step_size * h10 * scale, step_size * h11 * scale
    one, zero = jnp.ones_like(h00), jnp.zeros_like(h00)
    r00, r01, r02, r10, r11, r12 = one, zero, zero, zero, one, zero
    for degree in range(taylor_terms, 0, -1):
        part = 1.0 / degree
        r00, r01, r02, r10, r11, r12 = (
            one + (s00 * r00 + s01 * r10) * part,
            (s00 * r01 + s01 * r11) * part,
            (s00 * r02 + s01 * r12 + scale) * part,
            (s10 * r00 + s11 * r10) * part,
            one + (s10 * r01 + s11 * r11) * part,
            (s10 * r02 + s11 * r12) * part,
        )
    for repeat in range(squarings):
        r00, r01, r02, r10, r11, r12 = (
            r00 * r00 + r01 * r10,
            r00 * r01 + r01 * r11,
            r00 * r02 + r01 * r12 + r02,
            r10 * r00 + r11 * r10,
            r10 * r01 + r11 * r11,
            r10 * r02 + r11 * r12 + r12,
        )
    return r00, r10, r02, r12


def combined(step_size, partial_refs, scalars_ref, basis_ref):
    inner = partial_refs[0][...]
    for ref in partial_refs[1:]:
        inner = inner + ref[...]
    norm, first, length = scalars_ref[0], scalars_ref[1], scalars_ref[2]
    e0, e1, f0, f1 = exponential(step_size, first, inner[0], length, inner[1])

    def spread(value):
        return value[:, :1]

    carried = basis_ref[0] * spread(norm * e0) + basis_ref[1] * spread(norm * e1)
    forced = basis_ref[0] * spread(step_size * norm * f0) + basis_ref[1] * spread(
        step_size * norm * f1
    )
    return carried, forced


def start_kernel(sums, members, counts_ref, *refs):
    partial_refs, (scalars_ref, basis_ref, state_ref, local_ref) = refs[:sums], refs[sums:]
    step_size = counts_ref[0].astype(jnp.float32) * time_step
    carried, forced = combined(step_size, partial_refs, scalars_ref, basis_ref)
    local_ref[...] = forced[members:]
    state_ref[...] = carried[:members] + forced[members:]


def next_kernel(sums, counts_ref, *refs):
    partial_refs, (scalars_ref, basis_ref, local_ref, state_ref) = refs[:sums], refs[sums:]
    step_size = counts_ref[0].astype(jnp.float32) * time_step
    carried, _ = combined(step_size, partial_refs, scalars_ref, basis_ref)
    state_ref[...] = carried + local_ref[...]


def permuted(array, tm_change, row_change):
    sections, devices = lax.axis_size("tm"), lax.axis_size("row")
    pairs = [
        (s * devices + r, (s ^ tm_change) * devices + (r ^ row_change))
        for s in range(sections)
        for r in range(devices)
    ]
    return lax.ppermute(array, ("tm", "row"), pairs)


def gathered(own, tm_change=0):
    devices = lax.axis_size("row")
    blocks = []
    for change in range(0, devices, 2):
        if change == 0 and tm_change == 0:
            blocks.append(own)
        else:
            blocks.append(permuted(own, tm_change, change))
    near = jnp.stack(blocks)
    return near, permuted(near, 0, 1)


def summed(partial):
    devices = lax.axis_size("row")
    pair = partial + permuted(partial, 0, 1)
    return [pair] + [permuted(pair, 0, change) for change in range(2, devices, 2)]


def on_device(coupling, damping, forcing, initial, counts):
    local_coupling = coupling[0]
    local_forcing = forcing[0]
    members, rows = initial.shape
    extent = local_coupling.shape[1]
    devices = lax.axis_size("row")
    sections = lax.axis_size("tm")
    slab_index = lax.axis_index("tm")
    me = lax.axis_index("row").astype(jnp.int32).reshape(1)

    operator = load_operator(local_coupling, me, devices)

    def scratch(batch):
        return [
            pltpu.VMEM((devices, 2 * batch, rows), jnp.float32),
            pltpu.VMEM((2 * batch, rows), jnp.float32),
        ]

    def cost(batch):
        return pl.CostEstimate(
            flops=16 * rows * extent, bytes_accessed=4 * rows * extent, transcendentals=0
        )

    params = pltpu.CompilerParams(vmem_limit_bytes=12 * MIB)

    def first_pass(xa, xb):
        batch = xa.shape[1]
        return pl.pallas_call(
            first_kernel,
            out_shape=jax.ShapeDtypeStruct((batch, rows), jnp.float32),
            in_specs=[VMEM] * (3 + PIECES),
            out_specs=VMEM,
            scratch_shapes=scratch(batch),
            compiler_params=params,
            cost_estimate=cost(batch),
            name="first_pass",
        )(xa, xb, damping, *operator)

    def second_pass(xa, xb, wa, wb):
        batch = xa.shape[1]
        return pl.pallas_call(
            second_kernel,
            out_shape=(
                jax.ShapeDtypeStruct((2, batch, 128), jnp.float32),
                jax.ShapeDtypeStruct((3, batch, 128), jnp.float32),
                jax.ShapeDtypeStruct((2, batch, rows), jnp.float32),
            ),
            in_specs=[VMEM] * (5 + PIECES),
            out_specs=(VMEM,) * 3,
            scratch_shapes=scratch(batch),
            compiler_params=params,
            cost_estimate=cost(batch),
            name="second_pass",
        )(xa, xb, wa, wb, damping, *operator)

    small = jax.ShapeDtypeStruct((members, rows), jnp.float32)
    xa, xb = gathered(jnp.concatenate([initial, local_forcing], axis=0))
    wa, wb = gathered(first_pass(xa, xb))
    partial, scalars, basis = second_pass(xa, xb, wa, wb)
    parts = summed(partial)
    state, local = pl.pallas_call(
        functools.partial(start_kernel, len(parts), members),
        out_shape=(small, small),
        in_specs=[SMEM] + [VMEM] * (len(parts) + 2),
        out_specs=(VMEM, VMEM),
        compiler_params=params,
        name="start_state",
    )(counts, *parts, scalars, basis)
    result = state
    for section in range(1, sections):
        xa, xb = gathered(state, (section - 1) ^ section)
        wa, wb = gathered(first_pass(xa, xb))
        partial, scalars, basis = second_pass(xa, xb, wa, wb)
        parts = summed(partial)
        state = pl.pallas_call(
            functools.partial(next_kernel, len(parts)),
            out_shape=small,
            in_specs=[SMEM] + [VMEM] * (len(parts) + 3),
            out_specs=VMEM,
            compiler_params=params,
            name="next_state",
        )(counts, *parts, scalars, basis, local)
        result = jnp.where(slab_index == section, state, result)
    return result[None]


def solution(mesh):
    placed = (P("tm", "row", None), P("tm", "row"), P("tm", None, "row"), P(None, "row"), P("tm"))
    return jax.shard_map(
        on_device, mesh=mesh, in_specs=placed, out_specs=P("tm", None, "row"), check_vma=False
    )
```

```python
import functools

import jax
import jax.numpy as jnp
from jax import lax
from jax.experimental import pallas as pl
from jax.experimental.pallas import tpu as pltpu
from jax.sharding import PartitionSpec as P


time_step = 0.125
epsilon = 1e-06
squarings = 5
taylor_terms = 12
MIB = 1 << 20
VMEM = pl.BlockSpec(memory_space=pltpu.VMEM)
SMEM = pl.BlockSpec(memory_space=pltpu.SMEM)
ANY = pl.BlockSpec(memory_space=pl.ANY)
LOAD_WIDTH = 256
LOAD_SLOTS = 8
PIECES = 4


def load_kernel(devices, me_ref, a_ref, *refs):
    piece_refs, (slots, sems) = refs[:PIECES], refs[PIECES:]
    _, extent = a_ref.shape
    width = slots.shape[2]
    block = extent // devices
    per_block = block // width
    steps = extent // width
    half = devices // 2
    me = me_ref[0]

    def source(step):
        place = step // per_block
        offset = jnp.where(place < half, 2 * place, 2 * (place - half) + 1)
        owner = jnp.bitwise_xor(me, offset)
        start = owner * block + (step % per_block) * width
        return a_ref.at[:, pl.ds(pl.multiple_of(start, width), width)]

    def copy(step):
        slot = step % LOAD_SLOTS
        return pltpu.make_async_copy(source(step), slots.at[slot], sems.at[slot])

    for step in range(min(LOAD_SLOTS, steps)):
        copy(step).start()

    per_piece = steps // PIECES
    for piece, piece_ref in enumerate(piece_refs):

        @pl.loop(0, per_piece)
        def _(inner):
            step = inner + piece * per_piece
            copy(step).wait()
            turned = slots[step % LOAD_SLOTS].T
            high = turned.astype(jnp.bfloat16)
            place = pl.ds(pl.multiple_of(inner * width, width), width)
            piece_ref[0, place, :] = high
            piece_ref[1, place, :] = (turned - high.astype(jnp.float32)).astype(jnp.bfloat16)

            @pl.when(step + LOAD_SLOTS < steps)
            def _():
                copy(step + LOAD_SLOTS).start()


def load_operator(local_coupling, me, devices):
    rows, extent = local_coupling.shape
    width = min(LOAD_WIDTH, extent // devices)

    return pl.pallas_call(
        functools.partial(load_kernel, devices),
        out_shape=(pltpu.VMEM((2, extent // PIECES, rows), jnp.bfloat16),) * PIECES,
        in_specs=[SMEM, ANY],
        out_specs=(VMEM,) * PIECES,
        scratch_shapes=[
            pltpu.VMEM((LOAD_SLOTS, rows, width), jnp.float32),
            pltpu.SemaphoreType.DMA((LOAD_SLOTS,)),
        ],
        compiler_params=pltpu.CompilerParams(vmem_limit_bytes=12 * MIB),
        cost_estimate=pl.CostEstimate(
            flops=1600 * rows * extent, bytes_accessed=4 * rows * extent, transcendentals=0
        ),
        name="load_operator",
    )(me, local_coupling)


def apply_rows(blocks, places, piece_refs, split_ref, total_ref):
    members, width = blocks[0].shape
    per_piece = piece_refs[0].shape[1] // width
    total_ref[...] = jnp.zeros_like(total_ref)
    for index, (block, place) in enumerate(zip(blocks, places)):
        high = block.astype(jnp.bfloat16).astype(jnp.float32)
        split_ref[index, :members] = high
        split_ref[index, members:] = block - high
    for index, place in enumerate(places):
        piece_ref = piece_refs[place // per_piece]
        inside = pl.ds(place % per_piece * width, width)
        lhs = split_ref[index].astype(jnp.bfloat16)
        total_ref[...] += jnp.dot(
            lhs, piece_ref[0, inside, :], preferred_element_type=jnp.float32
        ) + jnp.dot(lhs, piece_ref[1, inside, :], preferred_element_type=jnp.float32)
    return total_ref[:members] + total_ref[members:]


def inner_product(first, second):
    return jnp.sum(jnp.sum(first * second, axis=0), axis=-1, keepdims=True)


def widened(value):
    return jnp.broadcast_to(value, (value.shape[0], 128))


def first_early(places, *refs):
    count = len(places)
    x_refs, piece_refs = refs[:count], refs[count:-3]
    out_ref, split_ref, total_ref = refs[-3:]
    out_ref[...] = apply_rows(
        [ref[...] for ref in x_refs], places, piece_refs, split_ref, total_ref
    )


def first_near(places, xa_ref, begun_ref, *refs):
    piece_refs, (out_ref, split_ref, total_ref) = refs[:-3], refs[-3:]
    blocks = [xa_ref[place] for place in places]
    out_ref[...] = begun_ref[...] + apply_rows(blocks, places, piece_refs, split_ref, total_ref)


def first_far(xa_ref, xb_ref, begun_ref, damping_ref, *refs):
    piece_refs, (image_ref, norm_ref, split_ref, total_ref) = refs[:-4], refs[-4:]
    xa, xb = xa_ref[...], xb_ref[...]
    norm = jnp.sqrt(inner_product(xa, xa) + inner_product(xb, xb) + epsilon)
    blocks = list(xb)
    image = begun_ref[...] + apply_rows(
        blocks, range(len(blocks)), piece_refs, split_ref, total_ref
    )
    image_ref[...] = (image - damping_ref[...] * xa[0]) / norm
    norm_ref[...] = widened(norm)


def second_early(places, xa_ref, norm_ref, *refs):
    count = len(places)
    w_refs, piece_refs = refs[:count], refs[count:-4]
    out_ref, estimate_ref, split_ref, total_ref = refs[-4:]
    q = [xa_ref[place] / norm_ref[:, :1] for place in places]
    w = [ref[...] for ref in w_refs]

    def inner(first, second):
        return sum(jnp.sum(x * y, axis=-1, keepdims=True) for x, y in zip(first, second))

    estimate = inner(q, w) / (inner(q, q) + epsilon)
    blocks = [x - estimate * y for x, y in zip(w, q)]
    out_ref[...] = apply_rows(blocks, places, piece_refs, split_ref, total_ref)
    estimate_ref[...] = widened(estimate)


def second_near(places, xa_ref, wa_ref, norm_ref, begun_ref, estimate_ref, *refs):
    piece_refs, (out_ref, split_ref, total_ref) = refs[:-3], refs[-3:]
    norm, estimate = norm_ref[:, :1], estimate_ref[:, :1]
    blocks = [wa_ref[place] - estimate * (xa_ref[place] / norm) for place in places]
    out_ref[...] = begun_ref[...] + apply_rows(blocks, places, piece_refs, split_ref, total_ref)


def second_far(
    xa_ref, xb_ref, wa_ref, wb_ref, norm_ref, begun_ref, estimate_ref, damping_ref, *refs
):
    piece_refs, refs = refs[:-5], refs[-5:]
    partial_ref, scalars_ref, basis_ref, split_ref, total_ref = refs
    wa, wb = wa_ref[...], wb_ref[...]
    norm, estimate = norm_ref[:, :1], estimate_ref[:, :1]
    qa, qb = xa_ref[...] / norm[None], xb_ref[...] / norm[None]
    blocks = list(wb - estimate[None] * qb)
    image = begun_ref[...] + apply_rows(
        blocks, range(len(blocks)), piece_refs, split_ref, total_ref
    )
    first = inner_product(qa, wa) + inner_product(qb, wb)
    ra, rb = wa - first[None] * qa, wb - first[None] * qb
    length = jnp.sqrt(inner_product(ra, ra) + inner_product(rb, rb) + epsilon)
    damping = damping_ref[...]
    image = image + (estimate - first) * (wa[0] + damping * qa[0])
    second = ra[0] / length
    image = image / length - damping * second
    for row, own in ((0, qa[0]), (1, second)):
        partial_ref[row] = widened(jnp.sum(own * image, axis=-1, keepdims=True))
        basis_ref[row] = own
    for row, value in enumerate((norm, first, length)):
        scalars_ref[row] = widened(value)


def exponential(step_size, h00, h01, h10, h11):
    scale = 1.0 / 2.0**squarings
    s00, s01 = step_size * h00 * scale, step_size * h01 * scale
    s10, s11 = step_size * h10 * scale, step_size * h11 * scale
    one, zero = jnp.ones_like(h00), jnp.zeros_like(h00)
    r00, r01, r02, r10, r11, r12 = one, zero, zero, zero, one, zero
    for degree in range(taylor_terms, 0, -1):
        part = 1.0 / degree
        r00, r01, r02, r10, r11, r12 = (
            one + (s00 * r00 + s01 * r10) * part,
            (s00 * r01 + s01 * r11) * part,
            (s00 * r02 + s01 * r12 + scale) * part,
            (s10 * r00 + s11 * r10) * part,
            one + (s10 * r01 + s11 * r11) * part,
            (s10 * r02 + s11 * r12) * part,
        )
    for _ in range(squarings):
        r00, r01, r02, r10, r11, r12 = (
            r00 * r00 + r01 * r10,
            r00 * r01 + r01 * r11,
            r00 * r02 + r01 * r12 + r02,
            r10 * r00 + r11 * r10,
            r10 * r01 + r11 * r11,
            r10 * r02 + r11 * r12 + r12,
        )
    return r00, r10, r02, r12


def combined(step_size, partial_refs, scalars_ref, basis_ref):
    inner = partial_refs[0][...]
    for ref in partial_refs[1:]:
        inner = inner + ref[...]
    norm, first, length = scalars_ref[0], scalars_ref[1], scalars_ref[2]
    e0, e1, f0, f1 = exponential(step_size, first, inner[0], length, inner[1])

    def spread(value):
        return value[:, :1]

    carried = basis_ref[0] * spread(norm * e0) + basis_ref[1] * spread(norm * e1)
    forced = basis_ref[0] * spread(step_size * norm * f0) + basis_ref[1] * spread(
        step_size * norm * f1
    )
    return carried, forced


def start_kernel(sums, members, counts_ref, *refs):
    partial_refs, (scalars_ref, basis_ref, state_ref, local_ref) = refs[:sums], refs[sums:]
    step_size = counts_ref[0].astype(jnp.float32) * time_step
    carried, forced = combined(step_size, partial_refs, scalars_ref, basis_ref)
    local_ref[...] = forced[members:]
    state_ref[...] = carried[:members] + forced[members:]


def next_kernel(sums, counts_ref, *refs):
    partial_refs, (scalars_ref, basis_ref, local_ref, state_ref) = refs[:sums], refs[sums:]
    step_size = counts_ref[0].astype(jnp.float32) * time_step
    carried, _ = combined(step_size, partial_refs, scalars_ref, basis_ref)
    state_ref[...] = carried + local_ref[...]


def permuted(array, tm_change, row_change):
    sections, devices = lax.axis_size("tm"), lax.axis_size("row")
    pairs = [
        (s * devices + r, (s ^ tm_change) * devices + (r ^ row_change))
        for s in range(sections)
        for r in range(devices)
    ]
    return lax.ppermute(array, ("tm", "row"), pairs)


def scattered(array, tm_change=0):
    devices = lax.axis_size("row")
    arrived = {0: array}
    for change in reversed(range(0 if tm_change else 2, devices, 2)):
        arrived[change] = permuted(array, tm_change, change)
    return [arrived[change] for change in range(0, devices, 2)]


def gathered(own, tm_change=0):
    blocks = scattered(own, tm_change)
    near = jnp.stack(blocks)
    return blocks, near, permuted(near, 0, 1)


def summed(partial):
    pair = partial + permuted(partial, 0, 1)
    return scattered(pair)


def on_device(coupling, damping, forcing, initial, counts):
    local_coupling = coupling[0]
    local_forcing = forcing[0]
    members, rows = initial.shape
    extent = local_coupling.shape[1]
    devices = lax.axis_size("row")
    sections = lax.axis_size("tm")
    slab_index = lax.axis_index("tm")
    me = lax.axis_index("row").astype(jnp.int32).reshape(1)

    operator = load_operator(local_coupling, me, devices)

    params = pltpu.CompilerParams(vmem_limit_bytes=8 * MIB)
    near_pieces, far_pieces = operator[: PIECES // 2], operator[PIECES // 2 :]

    def part_pass(kernel, outs, *inputs):
        batch = outs[0][-2]
        return pl.pallas_call(
            kernel,
            out_shape=tuple(jax.ShapeDtypeStruct(shape, jnp.float32) for shape in outs),
            in_specs=[VMEM] * len(inputs),
            out_specs=(VMEM,) * len(outs),
            scratch_shapes=[
                pltpu.VMEM((devices // 2, 2 * batch, rows), jnp.float32),
                pltpu.VMEM((2 * batch, rows), jnp.float32),
            ],
            compiler_params=params,
            cost_estimate=pl.CostEstimate(
                flops=16 * rows * extent, bytes_accessed=rows * extent, transcendentals=0
            ),
        )(*inputs)

    def krylov_step(own, finish, tm_change=0):
        batch = own.shape[0]
        block, lane = (batch, rows), (batch, 128)
        places = range(devices // 2)
        early = [places[-1], places[-2] if tm_change else 0]
        late = [place for place in places if place not in early]
        blocks, xa, xb = gathered(own, tm_change)
        (begun,) = part_pass(
            functools.partial(first_early, early), (block,),
            *[blocks[place] for place in early], *near_pieces,
        )
        (begun,) = part_pass(functools.partial(first_near, late), (block,), xa, begun, *near_pieces)
        image, norm = part_pass(first_far, (block, lane), xa, xb, begun, damping, *far_pieces)
        early = [places[-1], 0]
        late = [place for place in places if place not in early]
        blocks, wa, wb = gathered(image)
        begun, estimate = part_pass(
            functools.partial(second_early, early), (block, lane),
            xa, norm, *[blocks[place] for place in early], *near_pieces,
        )
        (begun,) = part_pass(
            functools.partial(second_near, late), (block,),
            xa, wa, norm, begun, estimate, *near_pieces,
        )
        partial, scalars, basis = part_pass(
            second_far, ((2, *lane), (3, *lane), (2, *block)),
            xa, xb, wa, wb, norm, begun, estimate, damping, *far_pieces,
        )
        return finish(summed(partial), scalars, basis)

    small = jax.ShapeDtypeStruct((members, rows), jnp.float32)

    def start(parts, scalars, basis):
        return pl.pallas_call(
            functools.partial(start_kernel, len(parts), members),
            out_shape=(small, small),
            in_specs=[SMEM] + [VMEM] * (len(parts) + 2),
            out_specs=(VMEM, VMEM),
            compiler_params=params,
            name="start_state",
        )(counts, *parts, scalars, basis)

    def follow(parts, scalars, basis):
        return pl.pallas_call(
            functools.partial(next_kernel, len(parts)),
            out_shape=small,
            in_specs=[SMEM] + [VMEM] * (len(parts) + 3),
            out_specs=VMEM,
            compiler_params=params,
            name="next_state",
        )(counts, *parts, scalars, basis, local)

    own = jnp.concatenate([initial, local_forcing], axis=0)
    state, local = krylov_step(own, start)
    result = state
    for section in range(1, sections):
        state = krylov_step(state, follow, (section - 1) ^ section)
        result = jnp.where(slab_index == section, state, result)
    return result[None]


def solution(mesh):
    placed = (P("tm", "row", None), P("tm", "row"), P("tm", None, "row"), P(None, "row"), P("tm"))
    return jax.shard_map(
        on_device, mesh=mesh, in_specs=placed, out_specs=P("tm", None, "row"), check_vma=False
    )
```
